8 devices in a mesh: dp: 8 (over z, y, x, core).
Axes of the slice: x: 2, y: 2, z: 1, core: 2. Of those that a mesh axis runs over, the one named last changes fastest.
Arguments:
- img_emb: bfloat16 [32768, 512], P('dp')
- txt_emb: bfloat16 [32768, 512], P('dp')
- log_temp: float32 [1], replicated
- logit_bias: float32 [1], replicated
Outputs:
- output 1: float32 [1], replicated
- output 2: float32 [32768, 512], P('dp')
- output 3: float32 [32768, 512], P('dp')
- output 4: float32 [1], replicated
- output 5: float32 [1], replicated
All inputs are finite; a program needn't handle non-finite values.
Results may differ from the reference program's by a relative error of at most 0.001.
Values are sent between devices in bfloat16 or wider.
A program may use at most 1 GiB of HBM per device.

```python
import math
import jax
import jax.numpy as jnp
from jax import lax

ROWS = 4096
DEVICES = 8
EMBED = 512
ROW_BLOCK = 64


def setup_inputs(seed: int = 0) -> dict:
    n_total = ROWS * DEVICES
    sub_keys = jax.random.split(jax.random.key(seed), 6)
    latent = jax.random.normal(sub_keys[0], (n_total, EMBED), jnp.float32)
    shard_shift = jax.random.randint(sub_keys[1], (n_total,), 1, DEVICES)
    partner = (jnp.arange(n_total) + shard_shift * ROWS) % n_total
    img_raw = latent + 0.5 * jax.random.normal(sub_keys[2], (n_total, EMBED), jnp.float32)
    txt_raw = latent + 0.8 * latent[partner] + 0.5 * jax.random.normal(sub_keys[3], (n_total, EMBED), jnp.float32)
    img_emb = img_raw / jnp.linalg.norm(img_raw, axis=1, keepdims=True)
    txt_emb = txt_raw / jnp.linalg.norm(txt_raw, axis=1, keepdims=True)
    log_temp = math.log(2.0 * math.log(n_total)) + jax.random.uniform(sub_keys[4], (1,), jnp.float32, -0.25, 0.25)
    logit_bias = -math.log(n_total) + jax.random.uniform(sub_keys[5], (1,), jnp.float32, -1.0, 1.0)
    return {'img_emb': img_emb.astype(jnp.bfloat16), 'txt_emb': txt_emb.astype(jnp.bfloat16), 'log_temp': log_temp, 'logit_bias': logit_bias}


def reference(img_emb, txt_emb, log_temp, logit_bias):
    n_total = img_emb.shape[0]
    n_blocks = n_total // ROW_BLOCK
    temp_scale = jnp.exp(log_temp[0])
    bias_val = logit_bias[0]
    col_ids = jnp.arange(n_total)
    img_blocks = img_emb.reshape(n_blocks, ROW_BLOCK, EMBED)

    def block_step(loop_state, step_in):
        loss_acc, bias_acc, temp_acc, txt_acc = loop_state
        block_idx, img_block = step_in
        row_ids = block_idx * ROW_BLOCK + jnp.arange(ROW_BLOCK)
        labels = jnp.where(row_ids[:, None] == col_ids[None, :], 1.0, -1.0)
        dot_vals = jnp.dot(img_block, txt_emb.T, preferred_element_type=jnp.float32)
        margin = labels * (temp_scale * dot_vals + bias_val)
        loss_acc = loss_acc + jnp.sum(jax.nn.softplus(-margin))
        grad_coef = -labels * jax.nn.sigmoid(-margin)
        coef_bf16 = grad_coef.astype(jnp.bfloat16)
        bias_acc = bias_acc + jnp.sum(grad_coef)
        temp_acc = temp_acc + jnp.sum(grad_coef * dot_vals)
        img_part = jnp.dot(coef_bf16, txt_emb, preferred_element_type=jnp.float32)
        txt_acc = txt_acc + jnp.dot(coef_bf16.T, img_block, preferred_element_type=jnp.float32)
        return (loss_acc, bias_acc, temp_acc, txt_acc), img_part

    zero_val = jnp.zeros((), jnp.float32)
    init_state = (zero_val, zero_val, zero_val, jnp.zeros((n_total, EMBED), jnp.float32))
    final_state, img_parts = lax.scan(block_step, init_state, (jnp.arange(n_blocks), img_blocks))
    loss_acc, bias_acc, temp_acc, txt_acc = final_state
    factor = temp_scale / n_total
    total_loss = (loss_acc / n_total).reshape(1)
    img_grad = img_parts.reshape(n_total, EMBED) * factor
    txt_grad = txt_acc * factor
    temp_grad = (temp_acc * factor).reshape(1)
    bias_grad = (bias_acc / n_total).reshape(1)
    return (total_loss, img_grad, txt_grad, temp_grad, bias_grad)
```

```python
import functools
import jax
import jax.numpy as jnp
from jax import lax
from jax.experimental import pallas as pl
from jax.experimental.pallas import tpu as pltpu
from jax.sharding import PartitionSpec as P

F32 = jnp.float32
BF16 = jnp.bfloat16
CLAMP = 31.0
LOG2E = 1.4426950408889634
LN2 = 0.6931471805599453
TILE = 1024
PIECE_M = 256
PIECE_N = 512
NN = (((1,), (0,)), ((), ()))
NT = (((1,), (1,)), ((), ()))
TN = (((0,), (0,)), ((), ()))


def dot(a, b, dims):
    return lax.dot_general(a, b, dims, preferred_element_type=F32)


def fold(x):
    m, n = x.shape
    x = jnp.sum(x.reshape(m // 8, 8, n), axis=0)
    return sum(x[:, k * 128:(k + 1) * 128] for k in range(n // 128))


def pair_terms(y, flip):
    if flip is not None:
        y = jnp.where(flip, -y, y)
    e = jnp.exp2(jnp.minimum(y, CLAMP))
    d = 1.0 + e
    c = e * (1.0 / d)
    h = e.shape[0] // 4
    e0, e1, e2, e3 = (e[k * h:(k + 1) * h] for k in range(4))
    qa = e0 * d[h:2 * h] + e1
    qb = e2 * d[3 * h:] + e3
    q = qa * (1.0 + qb) + qb
    dq = 1.0 + q
    log_part = jnp.log2(dq)
    rest_part = (q - (dq - 1.0)) * (1.0 / dq)
    if flip is not None:
        c = jnp.where(flip, -c, c)
    return c, log_part, rest_part


def block_kernel(sc_ref, img_ref, txt_ref, ig_in, tg_in, st_in, ig_ref, tg_ref, st_ref, coef, *, diag, img_outer, i0, j0):
    outer, inner = pl.program_id(0), pl.program_id(1)
    i, j = (outer, inner) if img_outer else (inner, outer)
    s2 = sc_ref[0]
    b2 = sc_ref[1]

    @pl.when((outer == 0) & (inner == 0))
    def _():
        st_ref[...] = st_in[...]

    keep_ref, keep_in = (ig_ref, ig_in) if img_outer else (tg_ref, tg_in)

    @pl.when(inner == 0)
    def _():
        keep_ref[...] = keep_in[...]

    tg_base = tg_in if img_outer else tg_ref
    ig_base = ig_ref if img_outer else ig_in

    def flip_mask(m, n, rows, cols):
        row = lax.broadcasted_iota(jnp.int32, (rows, cols), 0) + ((i0 + i) * TILE + m)
        col = lax.broadcasted_iota(jnp.int32, (rows, cols), 1) + ((j0 + j) * TILE + n)
        return row == col

    for n in range(0, TILE, PIECE_N):
        for m in range(0, TILE, PIECE_M):
            dots = dot(img_ref[m:m + PIECE_M, :], txt_ref[n:n + PIECE_N, :], NT)
            flip = flip_mask(m, n, PIECE_M, PIECE_N) if diag else None
            c, log_part, rest_part = pair_terms(dots * s2 + b2, flip)
            coef[m:m + PIECE_M, n:n + PIECE_N] = c.astype(BF16)
            st_ref[0] += fold(log_part)
            st_ref[1] += fold(rest_part)
            st_ref[2] += fold(c)
            st_ref[3] += fold(c * dots)
        tg_ref[n:n + PIECE_N, :] = tg_base[n:n + PIECE_N, :] + dot(coef[:, n:n + PIECE_N], img_ref[...], TN)
    ig_ref[...] = ig_base[...] + dot(coef[...], txt_ref[...], NN)

    @pl.when(sc_ref[2] > 0.0)
    def _():
        @pl.loop(0, TILE // 256)
        def _(k):
            m = pl.multiple_of(k * 256, 256)
            y = dot(img_ref[pl.ds(m, 256), :], txt_ref[...], NT) * s2 + b2
            if diag:
                y = jnp.where(flip_mask(m, 0, 256, TILE), 0.0, y)
            st_ref[0] += fold(jnp.maximum(y - CLAMP, 0.0))

    if diag:
        @pl.when((sc_ref[3] > 0.0) & (i0 + i == j0 + j))
        def _():
            own = jnp.sum(img_ref[...].astype(F32) * txt_ref[...].astype(F32), axis=1, keepdims=True)
            excess = jnp.maximum(-(own * s2 + b2) - CLAMP, 0.0)
            st_ref[0] += fold(jnp.broadcast_to(excess, (TILE, 128))) * (1.0 / 128.0)


def block_call(sc, img, txt, ig, tg, st, *, diag=False, img_outer=True, irange=None, jrange=None):
    dim = img.shape[1]
    i0, i1 = irange or (0, img.shape[0] // TILE)
    j0, j1 = jrange or (0, txt.shape[0] // TILE)
    ni, nj = i1 - i0, j1 - j0
    if img_outer:
        grid = (ni, nj)
        imap = lambda a, b: (a + i0, 0)
        jmap = lambda a, b: (b + j0, 0)
    else:
        grid = (nj, ni)
        imap = lambda a, b: (b + i0, 0)
        jmap = lambda a, b: (a + j0, 0)
    ispec = pl.BlockSpec((TILE, dim), imap)
    jspec = pl.BlockSpec((TILE, dim), jmap)
    sspec = pl.BlockSpec(st.shape, lambda a, b: (0, 0, 0))
    pairs = ni * nj * TILE * TILE
    return pl.pallas_call(
        functools.partial(block_kernel, diag=diag, img_outer=img_outer, i0=i0, j0=j0),
        grid=grid,
        in_specs=[pl.BlockSpec(memory_space=pltpu.SMEM), ispec, jspec, ispec, jspec, sspec],
        out_specs=[ispec, jspec, sspec],
        out_shape=[jax.ShapeDtypeStruct(ig.shape, F32), jax.ShapeDtypeStruct(tg.shape, F32), jax.ShapeDtypeStruct(st.shape, F32)],
        scratch_shapes=[pltpu.VMEM((TILE, TILE), BF16)],
        input_output_aliases={3: 0, 4: 1, 5: 2},
        compiler_params=pltpu.CompilerParams(dimension_semantics=("arbitrary", "arbitrary"), vmem_limit_bytes=48 * 2**20),
        cost_estimate=pl.CostEstimate(flops=6 * pairs * dim, transcendentals=3 * pairs, bytes_accessed=40 * 2**20),
        name="pair_block",
    )(sc, img, txt, ig, tg, st)


def solution(mesh):
    axis_name = mesh.axis_names[0]
    n_dev = mesh.shape[axis_name]

    def swap(x, bit):
        return lax.ppermute(x, axis_name, [(d, d ^ bit) for d in range(n_dev)])

    CORE, X, Y = 1, 2, 4

    def per_device(img_own, txt_own, log_temp, logit_bias):
        rows, dim = img_own.shape
        n_total = rows * n_dev
        nb = rows // TILE
        scale = jnp.exp(log_temp[0])
        bias = logit_bias[0]
        over = jnp.where(scale * 1.02 + bias > CLAMP * LN2, 1.0, 0.0)
        over_own = jnp.where(scale * 1.02 - bias > CLAMP * LN2, 1.0, 0.0)
        sc = jnp.stack([scale * LOG2E, bias * LOG2E, over, over_own]).astype(F32)

        txt_p = swap(txt_own, CORE)
        img_x = swap(img_own, X)
        txt_y = swap(txt_own, Y)
        txt_yp = swap(txt_y, CORE)

        zero = jnp.zeros((rows, dim), F32)
        st = jnp.zeros((4, 8, 128), F32)
        half = nb // 2

        ig_own, tg_own, st = block_call(sc, img_own, txt_own, zero, zero, st, diag=True)
        ig_own, tg_p, st = block_call(sc, img_own, txt_p, ig_own, zero, st, irange=(0, half // 2))
        ig_x, tg_yp, st = block_call(sc, img_x, txt_yp, zero, zero, st)
        ig_x, tg_y, st = block_call(sc, img_x, txt_y, ig_x, zero, st)
        ig_own, tg_yp, st = block_call(sc, img_own, txt_yp, ig_own, tg_yp, st)
        from_p_y = swap(tg_yp, CORE)
        ig_x, tg_own, st = block_call(sc, img_x, txt_own, ig_x, tg_own, st, irange=(0, half))
        ig_x, tg_p, st = block_call(sc, img_x, txt_p, ig_x, tg_p, st, irange=(0, half))
        cut = half * TILE
        from_x0 = swap(ig_x[:cut], X)
        ig_own, tg_y, st = block_call(sc, img_own, txt_y, ig_own, tg_y, st, img_outer=False, jrange=(0, half))
        from_y0 = swap(tg_y[:cut] + from_p_y[:cut], Y)
        ig_x, tg_own, st = block_call(sc, img_x, txt_own, ig_x, tg_own, st, irange=(half, nb))
        ig_x, tg_p, st = block_call(sc, img_x, txt_p, ig_x, tg_p, st, irange=(half, nb))
        from_x1 = swap(ig_x[cut:], X)
        ig_own, tg_y, st = block_call(sc, img_own, txt_y, ig_own, tg_y, st, img_outer=False, jrange=(half, nb))
        from_y1 = swap(tg_y[cut:] + from_p_y[cut:], Y)
        ig_own, tg_p, st = block_call(sc, img_own, txt_p, ig_own, tg_p, st, irange=(half // 2, nb))
        from_p = swap(tg_p, CORE)

        factor = scale / n_total
        img_grad = (ig_own + jnp.concatenate([from_x0, from_x1])) * factor
        txt_grad = (tg_own + from_p + jnp.concatenate([from_y0, from_y1])) * factor
        sums = jnp.sum(st, axis=(1, 2))
        sums = lax.psum(jnp.stack([sums[0] * LN2 + sums[1], sums[2], sums[3]]), axis_name)
        return (sums[0:1] / n_total, img_grad, txt_grad, sums[2:3] * factor, sums[1:2] / n_total)

    return jax.shard_map(per_device, mesh=mesh, in_specs=(P(axis_name, None), P(axis_name, None), P(None), P(None)), out_specs=(P(None), P(axis_name, None), P(axis_name, None), P(None), P(None)), check_vma=False)
```

```python
import functools
import jax
import jax.numpy as jnp
from jax import lax
from jax.experimental import pallas as pl
from jax.experimental.pallas import tpu as pltpu
from jax.sharding import PartitionSpec as P


F32 = jnp.float32
BF16 = jnp.bfloat16
CLAMP = 31.0
LOG2E = 1.4426950408889634
LN2 = 0.6931471805599453
TILE = 1024
PIECE_M = 256
PIECE_N = 512
NN = (((1,), (0,)), ((), ()))
NT = (((1,), (1,)), ((), ()))
TN = (((0,), (0,)), ((), ()))


def dot(a, b, dims):
    return lax.dot_general(a, b, dims, preferred_element_type=F32)


def fold(x):
    m, n = x.shape
    x = jnp.sum(x.reshape(m // 8, 8, n), axis=0)
    return sum(x[:, k * 128:(k + 1) * 128] for k in range(n // 128))


def pair_terms(y, flip):
    if flip is not None:
        y = jnp.where(flip, -y, y)
    e = jnp.exp2(jnp.minimum(y, CLAMP))
    d = 1.0 + e
    c = e * (1.0 / d)
    h = e.shape[0] // 4
    e0, e1, e2, e3 = (e[k * h:(k + 1) * h] for k in range(4))
    qa = e0 * d[h:2 * h] + e1
    qb = e2 * d[3 * h:] + e3
    q = qa * (1.0 + qb) + qb
    dq = 1.0 + q
    log_part = jnp.log2(dq)
    rest_part = (q - (dq - 1.0)) * (1.0 / dq)
    if flip is not None:
        c = jnp.where(flip, -c, c)
    return c, log_part, rest_part


def block_kernel(*refs, diag, img_outer, i0, j0, keep_init, extra, fresh_from):
    it = iter(refs)
    sc_ref, img_ref, txt_ref = next(it), next(it), next(it)
    stream_in = next(it)
    keep_in = next(it) if keep_init else None
    keep_extra = next(it) if extra else None
    st_in, stream_ref, keep_ref, st_ref, coef = it
    outer, inner = pl.program_id(0), pl.program_id(1)
    i, j = (outer, inner) if img_outer else (inner, outer)
    s2 = sc_ref[0]
    b2 = sc_ref[1]

    @pl.when((outer == 0) & (inner == 0))
    def _():
        st_ref[...] = st_in[...]

    @pl.when(inner == 0)
    def _():
        base = keep_in[...] if keep_init else jnp.zeros_like(keep_ref)
        keep_ref[...] = base + keep_extra[...] if extra else base

    if fresh_from is not None:
        @pl.when((outer == 0) & (inner >= fresh_from))
        def _():
            stream_in[...] = jnp.zeros_like(stream_in)

    if img_outer:
        ig_ref, tg_ref, ig_base, tg_base = keep_ref, stream_ref, keep_ref, stream_in
    else:
        ig_ref, tg_ref, ig_base, tg_base = stream_ref, keep_ref, stream_in, keep_ref

    def flip_mask(m, n, rows, cols):
        row = lax.broadcasted_iota(jnp.int32, (rows, cols), 0) + ((i0 + i) * TILE + m)
        col = lax.broadcasted_iota(jnp.int32, (rows, cols), 1) + ((j0 + j) * TILE + n)
        return row == col

    for n in range(0, TILE, PIECE_N):
        for m in range(0, TILE, PIECE_M):
            dots = dot(img_ref[m:m + PIECE_M, :], txt_ref[n:n + PIECE_N, :], NT)
            flip = flip_mask(m, n, PIECE_M, PIECE_N) if diag else None
            c, log_part, rest_part = pair_terms(dots * s2 + b2, flip)
            coef[m:m + PIECE_M, n:n + PIECE_N] = c.astype(BF16)
            st_ref[0] += fold(log_part)
            st_ref[1] += fold(rest_part)
            st_ref[2] += fold(c)
            st_ref[3] += fold(c * dots)
        tg_ref[n:n + PIECE_N, :] = tg_base[n:n + PIECE_N, :] + dot(coef[:, n:n + PIECE_N], img_ref[...], TN)
    ig_ref[...] = ig_base[...] + dot(coef[...], txt_ref[...], NN)

    @pl.when(sc_ref[2] > 0.0)
    def _():
        @pl.loop(0, TILE // 256)
        def _(k):
            m = pl.multiple_of(k * 256, 256)
            y = dot(img_ref[pl.ds(m, 256), :], txt_ref[...], NT) * s2 + b2
            if diag:
                y = jnp.where(flip_mask(m, 0, 256, TILE), 0.0, y)
            st_ref[0] += fold(jnp.maximum(y - CLAMP, 0.0))

    if diag:
        @pl.when((sc_ref[3] > 0.0) & (i0 + i == j0 + j))
        def _():
            own = jnp.sum(img_ref[...].astype(F32) * txt_ref[...].astype(F32), axis=1, keepdims=True)
            excess = jnp.maximum(-(own * s2 + b2) - CLAMP, 0.0)
            st_ref[0] += fold(jnp.broadcast_to(excess, (TILE, 128))) * (1.0 / 128.0)


def block_call(sc, img, txt, stream, keep, st, *, diag=False, img_outer=True, irange=None, jrange=None, keep_off=0, keep_rows=None, extra=None, fresh_from=None):
    dim = img.shape[1]
    i0, i1 = irange or (0, img.shape[0] // TILE)
    j0, j1 = jrange or (0, txt.shape[0] // TILE)
    ni, nj = i1 - i0, j1 - j0
    if img_outer:
        grid, o0, n0 = (ni, nj), i0, j0
    else:
        grid, o0, n0 = (nj, ni), j0, i0
    ospec = lambda off: pl.BlockSpec((TILE, dim), lambda a, b: (a + off, 0))
    nspec = lambda off: pl.BlockSpec((TILE, dim), lambda a, b: (b + off, 0))
    keep_rows = keep_rows or (img if img_outer else txt).shape[0]
    sspec = pl.BlockSpec(st.shape, lambda a, b: (0, 0, 0))
    in_specs = [pl.BlockSpec(memory_space=pltpu.SMEM)]
    in_specs += [ospec(i0), nspec(j0)] if img_outer else [nspec(i0), ospec(j0)]
    in_specs += [nspec(n0)]
    args = [sc, img, txt, stream]
    alias = {3: 0}
    out_off = o0 - keep_off
    if keep is not None:
        in_off = o0 if keep.shape[0] > keep_rows else out_off
        if keep.shape[0] == keep_rows:
            alias[len(args)] = 1
        args.append(keep)
        in_specs.append(ospec(in_off))
    if extra is not None:
        args.append(extra)
        in_specs.append(ospec(o0))
    alias[len(args)] = 2
    args.append(st)
    in_specs.append(sspec)
    pairs = ni * nj * TILE * TILE
    kernel = functools.partial(
        block_kernel, diag=diag, img_outer=img_outer, i0=i0, j0=j0, keep_init=keep is not None, extra=extra is not None, fresh_from=fresh_from
    )
    return pl.pallas_call(
        kernel,
        grid=grid,
        in_specs=in_specs,
        out_specs=[nspec(n0), ospec(out_off), sspec],
        out_shape=[
            jax.ShapeDtypeStruct(stream.shape, F32),
            jax.ShapeDtypeStruct((keep_rows, dim), F32),
            jax.ShapeDtypeStruct(st.shape, F32),
        ],
        scratch_shapes=[pltpu.VMEM((TILE, TILE), BF16)],
        input_output_aliases=alias,
        compiler_params=pltpu.CompilerParams(dimension_semantics=("arbitrary", "arbitrary"), vmem_limit_bytes=48 * 2**20),
        cost_estimate=pl.CostEstimate(flops=6 * pairs * dim, transcendentals=3 * pairs, bytes_accessed=40 * 2**20),
        name="pair_block",
    )(*args)


def solution(mesh):
    axis_name = mesh.axis_names[0]
    n_dev = mesh.shape[axis_name]

    def swap(x, bit):
        return lax.ppermute(x, axis_name, [(d, d ^ bit) for d in range(n_dev)])

    CORE, X, Y = 1, 2, 4

    def per_device(img_own, txt_own, log_temp, logit_bias):
        rows, dim = img_own.shape
        n_total = rows * n_dev
        nb = rows // TILE
        half = nb // 2
        cut = half * TILE
        scale = jnp.exp(log_temp[0])
        bias = logit_bias[0]
        over = jnp.where(scale * 1.02 + bias > CLAMP * LN2, 1.0, 0.0)
        over_own = jnp.where(scale * 1.02 - bias > CLAMP * LN2, 1.0, 0.0)
        sc = jnp.stack([scale * LOG2E, bias * LOG2E, over, over_own]).astype(F32)

        img_x = swap(img_own, X)
        txt_y = swap(txt_own, Y)
        txt_p = swap(txt_own, CORE)
        txt_yp = swap(txt_y, CORE)

        zero = jnp.zeros((rows, dim), F32)
        st = jnp.zeros((4, 8, 128), F32)
        back = dict(img_outer=False)

        tg_own, ig_own, st = block_call(sc, img_own, txt_own, zero, None, st, diag=True, irange=(0, 1), fresh_from=0)
        ig_own, tg_p, st = block_call(sc, img_own, txt_p, ig_own, None, st, fresh_from=1, **back)
        ig_x, tg_y, st = block_call(sc, img_x, txt_y, zero, None, st, fresh_from=0, **back)
        ig_x, tg_yp, st = block_call(sc, img_x, txt_yp, ig_x, None, st, **back)
        ig_own, tg_yp, st = block_call(sc, img_own, txt_yp, ig_own, tg_yp, st, **back)
        from_yp = swap(tg_yp, CORE)
        tg_own, ig_x0, st = block_call(sc, img_x, txt_own, tg_own, ig_x, st, irange=(0, half), keep_rows=cut)
        tg_p, ig_x0, st = block_call(sc, img_x, txt_p, tg_p, ig_x0, st, irange=(0, half), keep_rows=cut)
        from_x0 = swap(ig_x0, X)
        ig_own, tg_y0, st = block_call(sc, img_own, txt_y, ig_own, tg_y, st, jrange=(0, half), keep_rows=cut, extra=from_yp, **back)
        from_y0 = swap(tg_y0, Y)
        tg_own, ig_x1, st = block_call(sc, img_x, txt_own, tg_own, ig_x, st, irange=(half, nb), keep_rows=cut, keep_off=half)
        tg_p, ig_x1, st = block_call(sc, img_x, txt_p, tg_p, ig_x1, st, irange=(half, nb), keep_rows=cut, keep_off=half)
        from_x1 = swap(ig_x1, X)
        from_p = swap(tg_p, CORE)
        ig_own, tg_y1, st = block_call(sc, img_own, txt_y, ig_own, tg_y, st, jrange=(half, nb), keep_rows=cut, keep_off=half, extra=from_yp, **back)
        from_y1 = swap(tg_y1, Y)
        tg_own, ig_own, st = block_call(sc, img_own, txt_own, tg_own, ig_own, st, diag=True, irange=(1, nb))

        factor = scale / n_total
        img_grad = (ig_own + jnp.concatenate([from_x0, from_x1])) * factor
        txt_grad = (tg_own + from_p + jnp.concatenate([from_y0, from_y1])) * factor
        sums = jnp.sum(st, axis=(1, 2))
        sums = lax.psum(jnp.stack([sums[0] * LN2 + sums[1], sums[2], sums[3]]), axis_name)
        return (sums[0:1] / n_total, img_grad, txt_grad, sums[2:3] * factor, sums[1:2] / n_total)

    return jax.shard_map(per_device, mesh=mesh, in_specs=(P(axis_name, None), P(axis_name, None), P(None), P(None)), out_specs=(P(None), P(axis_name, None), P(axis_name, None), P(None), P(None)), check_vma=False)
```

```python
import functools
import jax
import jax.numpy as jnp
from jax import lax
from jax.experimental import pallas as pl
from jax.experimental.pallas import tpu as pltpu
from jax.sharding import PartitionSpec as P


F32 = jnp.float32
BF16 = jnp.bfloat16
CLAMP = 31.0
LOG2E = 1.4426950408889634
LN2 = 0.6931471805599453
TILE = 1024
PIECE_M = 256
PIECE_N = 512
NN = (((1,), (0,)), ((), ()))
NT = (((1,), (1,)), ((), ()))
TN = (((0,), (0,)), ((), ()))


def dot(a, b, dims):
    return lax.dot_general(a, b, dims, preferred_element_type=F32)


def fold(x):
    m, n = x.shape
    x = jnp.sum(x.reshape(m // 8, 8, n), axis=0)
    return sum(x[:, k * 128:(k + 1) * 128] for k in range(n // 128))


def pair_terms(y, flip):
    if flip is not None:
        y = jnp.where(flip, -y, y)
    e = jnp.exp2(jnp.minimum(y, CLAMP))
    d = 1.0 + e
    c = e * (1.0 / d)
    h = e.shape[0] // 4
    e0, e1, e2, e3 = (e[k * h:(k + 1) * h] for k in range(4))
    qa = e0 * d[h:2 * h] + e1
    qb = e2 * d[3 * h:] + e3
    q = qa * (1.0 + qb) + qb
    dq = 1.0 + q
    log_part = jnp.log2(dq)
    rest_part = (q - (dq - 1.0)) * (1.0 / dq)
    if flip is not None:
        c = jnp.where(flip, -c, c)
    return c, log_part, rest_part


def block_kernel(*refs, diag, img_outer, i0, j0, stream_init, keep_init, extra, fresh_from, spare):
    it = iter(refs)
    sc_ref, img_ref, txt_ref = next(it), next(it), next(it)
    stream_in = next(it) if stream_init else None
    keep_in = next(it) if keep_init else None
    keep_extra = next(it) if extra else None
    st_in, stream_ref, keep_ref, st_ref = next(it), next(it), next(it), next(it)
    if spare:
        next(it)
    coef = next(it)
    outer, inner = pl.program_id(0), pl.program_id(1)
    i, j = (outer, inner) if img_outer else (inner, outer)
    s2 = sc_ref[0]
    b2 = sc_ref[1]

    @pl.when((outer == 0) & (inner == 0))
    def _():
        st_ref[...] = st_in[...]

    @pl.when(inner == 0)
    def _():
        base = keep_in[...] if keep_init else jnp.zeros_like(keep_ref)
        keep_ref[...] = base + keep_extra[...] if extra else base

    if fresh_from is not None:
        @pl.when((outer == 0) & (inner >= fresh_from))
        def _():
            stream_in[...] = jnp.zeros_like(stream_in)

    if img_outer:
        ig_ref, tg_ref, ig_base, tg_base = keep_ref, stream_ref, keep_ref, stream_in
    else:
        ig_ref, tg_ref, ig_base, tg_base = stream_ref, keep_ref, stream_in, keep_ref

    def flip_mask(m, n, rows, cols):
        row = lax.broadcasted_iota(jnp.int32, (rows, cols), 0) + ((i0 + i) * TILE + m)
        col = lax.broadcasted_iota(jnp.int32, (rows, cols), 1) + ((j0 + j) * TILE + n)
        return row == col

    def txt_part(n, k):
        add = dot(coef[:, n:n + PIECE_N], img_ref[:, k:k + 256], TN)
        tg_ref[n:n + PIECE_N, k:k + 256] = add if tg_base is None else tg_base[n:n + PIECE_N, k:k + 256] + add

    queue = []
    for n in range(0, TILE, PIECE_N):
        for m in range(0, TILE, PIECE_M):
            dots = dot(img_ref[m:m + PIECE_M, :], txt_ref[n:n + PIECE_N, :], NT)
            flip = flip_mask(m, n, PIECE_M, PIECE_N) if diag else None
            c, log_part, rest_part = pair_terms(dots * s2 + b2, flip)
            coef[m:m + PIECE_M, n:n + PIECE_N] = c.astype(BF16)
            st_ref[0] += fold(log_part)
            st_ref[1] += fold(rest_part)
            st_ref[2] += fold(c)
            st_ref[3] += fold(c * dots)
            left = (TILE - m) // PIECE_M
            for _ in range((len(queue) + left - 1) // left):
                queue.pop(0)()
        queue += [functools.partial(txt_part, n, k) for k in range(0, img_ref.shape[1], 256)]
    for task in queue:
        task()
    ig_ref[...] = ig_base[...] + dot(coef[...], txt_ref[...], NN)

    @pl.when(sc_ref[2] > 0.0)
    def _():
        @pl.loop(0, TILE // 256)
        def _(k):
            m = pl.multiple_of(k * 256, 256)
            y = dot(img_ref[pl.ds(m, 256), :], txt_ref[...], NT) * s2 + b2
            if diag:
                y = jnp.where(flip_mask(m, 0, 256, TILE), 0.0, y)
            st_ref[0] += fold(jnp.maximum(y - CLAMP, 0.0))

    if diag:
        @pl.when((sc_ref[3] > 0.0) & (i0 + i == j0 + j))
        def _():
            own = jnp.sum(img_ref[...].astype(F32) * txt_ref[...].astype(F32), axis=1, keepdims=True)
            excess = jnp.maximum(-(own * s2 + b2) - CLAMP, 0.0)
            st_ref[0] += fold(jnp.broadcast_to(excess, (TILE, 128))) * (1.0 / 128.0)


def block_call(sc, img, txt, stream, keep, st, *, diag=False, img_outer=True, irange=None, jrange=None, keep_off=0, keep_rows=None, extra=None, fresh_from=None, spare=False):
    dim = img.shape[1]
    i0, i1 = irange or (0, img.shape[0] // TILE)
    j0, j1 = jrange or (0, txt.shape[0] // TILE)
    ni, nj = i1 - i0, j1 - j0
    if img_outer:
        grid, o0, n0 = (ni, nj), i0, j0
    else:
        grid, o0, n0 = (nj, ni), j0, i0
    ospec = lambda off: pl.BlockSpec((TILE, dim), lambda a, b: (a + off, 0))
    nspec = lambda off: pl.BlockSpec((TILE, dim), lambda a, b: (b + off, 0))
    keep_rows = keep_rows or (img if img_outer else txt).shape[0]
    sspec = pl.BlockSpec(st.shape, lambda a, b: (0, 0, 0))
    in_specs = [pl.BlockSpec(memory_space=pltpu.SMEM)]
    in_specs += [ospec(i0), nspec(j0)] if img_outer else [nspec(i0), ospec(j0)]
    args = [sc, img, txt]
    alias = {}
    if stream is not None:
        alias[len(args)] = 0
        args.append(stream)
        in_specs.append(nspec(n0))
    out_off = o0 - keep_off
    if keep is not None:
        in_off = o0 if keep.shape[0] > keep_rows else out_off
        if keep.shape[0] == keep_rows:
            alias[len(args)] = 1
        args.append(keep)
        in_specs.append(ospec(in_off))
    if extra is not None:
        args.append(extra)
        in_specs.append(ospec(o0))
    alias[len(args)] = 2
    args.append(st)
    in_specs.append(sspec)
    pairs = ni * nj * TILE * TILE
    kernel = functools.partial(
        block_kernel, diag=diag, img_outer=img_outer, i0=i0, j0=j0, stream_init=stream is not None,
        keep_init=keep is not None, extra=extra is not None, fresh_from=fresh_from, spare=spare,
    )
    stream_shape = jax.ShapeDtypeStruct((txt if img_outer else img).shape, F32)
    spare_specs = [pl.BlockSpec(memory_space=pl.ANY)] if spare else []
    spare_shapes = [stream_shape] if spare else []
    return pl.pallas_call(
        kernel,
        grid=grid,
        in_specs=in_specs,
        out_specs=[nspec(n0), ospec(out_off), sspec] + spare_specs,
        out_shape=[
            stream_shape,
            jax.ShapeDtypeStruct((keep_rows, dim), F32),
            jax.ShapeDtypeStruct(st.shape, F32),
        ] + spare_shapes,
        scratch_shapes=[pltpu.VMEM((TILE, TILE), BF16)],
        input_output_aliases=alias,
        compiler_params=pltpu.CompilerParams(dimension_semantics=("arbitrary", "arbitrary"), vmem_limit_bytes=63 * 2**20),
        cost_estimate=pl.CostEstimate(flops=6 * pairs * dim, transcendentals=3 * pairs, bytes_accessed=40 * 2**20),
        name="pair_block",
    )(*args)


def solution(mesh):
    axis_name = mesh.axis_names[0]
    n_dev = mesh.shape[axis_name]

    def swap(x, bit):
        return lax.ppermute(x, axis_name, [(d, d ^ bit) for d in range(n_dev)])

    CORE, X, Y = 1, 2, 4

    def per_device(img_own, txt_own, log_temp, logit_bias):
        rows, _ = img_own.shape
        n_total = rows * n_dev
        nb = rows // TILE
        half = nb // 2
        cut = half * TILE
        scale = jnp.exp(log_temp[0])
        bias = logit_bias[0]
        over = jnp.where(scale * 1.02 + bias > CLAMP * LN2, 1.0, 0.0)
        over_own = jnp.where(scale * 1.02 - bias > CLAMP * LN2, 1.0, 0.0)
        sc = jnp.stack([scale * LOG2E, bias * LOG2E, over, over_own]).astype(F32)

        img_x = swap(img_own, X)
        txt_y = swap(txt_own, Y)
        txt_p = swap(txt_own, CORE)
        txt_yp = swap(txt_y, CORE)

        st = jnp.zeros((4, 8, 128), F32)
        back = dict(img_outer=False)

        tg_own, ig_own, st, spare = block_call(sc, img_own, txt_own, None, None, st, diag=True, irange=(0, 1), spare=True)
        ig_own, tg_p, st = block_call(sc, img_own, txt_p, ig_own, None, st, fresh_from=1, **back)
        ig_x, tg_y, st = block_call(sc, img_x, txt_y, spare, None, st, fresh_from=0, **back)
        ig_x, tg_yp, st = block_call(sc, img_x, txt_yp, ig_x, None, st, **back)
        ig_own, tg_yp, st = block_call(sc, img_own, txt_yp, ig_own, tg_yp, st, **back)
        from_yp = swap(tg_yp, CORE)
        tg_own, ig_x0, st = block_call(sc, img_x, txt_own, tg_own, ig_x, st, irange=(0, half), keep_rows=cut)
        tg_p, ig_x0, st = block_call(sc, img_x, txt_p, tg_p, ig_x0, st, irange=(0, half), keep_rows=cut)
        from_x0 = swap(ig_x0, X)
        ig_own, tg_y0, st = block_call(sc, img_own, txt_y, ig_own, tg_y, st, jrange=(0, half), keep_rows=cut, extra=from_yp, **back)
        from_y0 = swap(tg_y0, Y)
        tg_own, ig_x1, st = block_call(sc, img_x, txt_own, tg_own, ig_x, st, irange=(half, nb), keep_rows=cut, keep_off=half)
        tg_p, ig_x1, st = block_call(sc, img_x, txt_p, tg_p, ig_x1, st, irange=(half, nb), keep_rows=cut, keep_off=half)
        from_x1 = swap(ig_x1, X)
        from_p = swap(tg_p, CORE)
        last = cut - TILE
        ig_own, tg_y1, st = block_call(sc, img_own, txt_y, ig_own, tg_y, st, jrange=(half, nb - 1), keep_rows=last, keep_off=half, extra=from_yp, **back)
        from_y1 = swap(tg_y1, Y)
        ig_own, tg_y2, st = block_call(sc, img_own, txt_y, ig_own, tg_y, st, jrange=(nb - 1, nb), keep_rows=TILE, keep_off=nb - 1, extra=from_yp, **back)
        from_y2 = swap(tg_y2, Y)
        tg_own, ig_own, st = block_call(sc, img_own, txt_own, tg_own, ig_own, st, diag=True, irange=(1, nb))

        factor = scale / n_total
        img_grad = (ig_own + jnp.concatenate([from_x0, from_x1])) * factor
        txt_grad = (tg_own + from_p + jnp.concatenate([from_y0, from_y1, from_y2])) * factor
        sums = jnp.sum(st, axis=(1, 2))
        sums = lax.psum(jnp.stack([sums[0] * LN2 + sums[1], sums[2], sums[3]]), axis_name)
        return (sums[0:1] / n_total, img_grad, txt_grad, sums[2:3] * factor, sums[1:2] / n_total)

    return jax.shard_map(per_device, mesh=mesh, in_specs=(P(axis_name, None), P(axis_name, None), P(None), P(None)), out_specs=(P(None), P(axis_name, None), P(axis_name, None), P(None), P(None)), check_vma=False)
```

```python
import functools
import jax
import jax.numpy as jnp
from jax import lax
from jax.experimental import pallas as pl
from jax.experimental.pallas import tpu as pltpu
from jax.sharding import PartitionSpec as P


F32 = jnp.float32
BF16 = jnp.bfloat16
CLAMP = 31.0
LOG2E = 1.4426950408889634
LN2 = 0.6931471805599453
TILE = 1024
PIECE_M = 256
PIECE_N = 512
NN = (((1,), (0,)), ((), ()))
NT = (((1,), (1,)), ((), ()))
TN = (((0,), (0,)), ((), ()))


def dot(a, b, dims):
    return lax.dot_general(a, b, dims, preferred_element_type=F32)


def fold(x):
    m, n = x.shape
    x = jnp.sum(x.reshape(m // 8, 8, n), axis=0)
    return sum(x[:, k * 128:(k + 1) * 128] for k in range(n // 128))


def pair_terms(y, flip):
    if flip is not None:
        y = jnp.where(flip, -y, y)
    e = jnp.exp2(jnp.minimum(y, CLAMP))
    d = 1.0 + e
    c = e * (1.0 / d)
    h = e.shape[0] // 4
    e0, e1, e2, e3 = (e[k * h:(k + 1) * h] for k in range(4))
    qa = e0 * d[h:2 * h] + e1
    qb = e2 * d[3 * h:] + e3
    q = qa * (1.0 + qb) + qb
    dq = 1.0 + q
    log_part = jnp.log2(dq)
    rest_part = (q - (dq - 1.0)) * (1.0 / dq)
    if flip is not None:
        c = jnp.where(flip, -c, c)
    return c, log_part, rest_part


def block_kernel(*refs, diag, img_outer, i0, j0, stream_init, keep_init, extra, fresh_from, spare):
    it = iter(refs)
    sc_ref, img_ref, txt_ref = next(it), next(it), next(it)
    stream_in = next(it) if stream_init else None
    keep_in = next(it) if keep_init else None
    keep_extra = next(it) if extra else None
    st_in, stream_ref, keep_ref, st_ref = next(it), next(it), next(it), next(it)
    if spare:
        next(it)
    coef = next(it)
    outer, inner = pl.program_id(0), pl.program_id(1)
    i, j = (outer, inner) if img_outer else (inner, outer)
    s2 = sc_ref[0]
    b2 = sc_ref[1]

    @pl.when((outer == 0) & (inner == 0))
    def _():
        st_ref[...] = st_in[...]

    @pl.when(inner == 0)
    def _():
        base = keep_in[...] if keep_init else jnp.zeros_like(keep_ref)
        keep_ref[...] = base + keep_extra[...] if extra else base

    if fresh_from is not None:
        @pl.when((outer == 0) & (inner >= fresh_from))
        def _():
            stream_in[...] = jnp.zeros_like(stream_in)

    if img_outer:
        ig_ref, tg_ref, ig_base, tg_base = keep_ref, stream_ref, keep_ref, stream_in
    else:
        ig_ref, tg_ref, ig_base, tg_base = stream_ref, keep_ref, stream_in, keep_ref

    def flip_mask(m, n, rows, cols):
        row = lax.broadcasted_iota(jnp.int32, (rows, cols), 0) + ((i0 + i) * TILE + m)
        col = lax.broadcasted_iota(jnp.int32, (rows, cols), 1) + ((j0 + j) * TILE + n)
        return row == col

    def txt_part(n, k):
        add = dot(coef[:, n:n + PIECE_N], img_ref[:, k:k + 256], TN)
        tg_ref[n:n + PIECE_N, k:k + 256] = add if tg_base is None else tg_base[n:n + PIECE_N, k:k + 256] + add

    def tile(on_diag):
        queue = []
        for n in range(0, TILE, PIECE_N):
            for m in range(0, TILE, PIECE_M):
                dots = dot(img_ref[m:m + PIECE_M, :], txt_ref[n:n + PIECE_N, :], NT)
                flip = None
                if on_diag and m < n + PIECE_N and n < m + PIECE_M:
                    shape = (PIECE_M, PIECE_N)
                    flip = lax.broadcasted_iota(jnp.int32, shape, 0) + (m - n) == lax.broadcasted_iota(jnp.int32, shape, 1)
                c, log_part, rest_part = pair_terms(dots * s2 + b2, flip)
                coef[m:m + PIECE_M, n:n + PIECE_N] = c.astype(BF16)
                st_ref[0] += fold(log_part)
                st_ref[1] += fold(rest_part)
                st_ref[2] += fold(c)
                st_ref[3] += fold(c * dots)
                left = (TILE - m) // PIECE_M
                for _ in range((len(queue) + left - 1) // left):
                    queue.pop(0)()
            queue += [functools.partial(txt_part, n, k) for k in range(0, img_ref.shape[1], 256)]
        for task in queue:
            task()
        ig_ref[...] = ig_base[...] + dot(coef[...], txt_ref[...], NN)

    if diag:
        pl.when(i0 + i == j0 + j)(lambda: tile(True))
        pl.when(i0 + i != j0 + j)(lambda: tile(False))
    else:
        tile(False)

    @pl.when(sc_ref[2] > 0.0)
    def _():
        @pl.loop(0, TILE // 256)
        def _(k):
            m = pl.multiple_of(k * 256, 256)
            y = dot(img_ref[pl.ds(m, 256), :], txt_ref[...], NT) * s2 + b2
            if diag:
                y = jnp.where(flip_mask(m, 0, 256, TILE), 0.0, y)
            st_ref[0] += fold(jnp.maximum(y - CLAMP, 0.0))

    if diag:
        @pl.when((sc_ref[3] > 0.0) & (i0 + i == j0 + j))
        def _():
            own = jnp.sum(img_ref[...].astype(F32) * txt_ref[...].astype(F32), axis=1, keepdims=True)
            excess = jnp.maximum(-(own * s2 + b2) - CLAMP, 0.0)
            st_ref[0] += fold(jnp.broadcast_to(excess, (TILE, 128))) * (1.0 / 128.0)


def block_call(sc, img, txt, stream, keep, st, *, diag=False, img_outer=True, irange=None, jrange=None, keep_off=0, keep_rows=None, extra=None, fresh_from=None, spare=False):
    dim = img.shape[1]
    i0, i1 = irange or (0, img.shape[0] // TILE)
    j0, j1 = jrange or (0, txt.shape[0] // TILE)
    ni, nj = i1 - i0, j1 - j0
    if img_outer:
        grid, o0, n0 = (ni, nj), i0, j0
    else:
        grid, o0, n0 = (nj, ni), j0, i0
    ospec = lambda off: pl.BlockSpec((TILE, dim), lambda a, b: (a + off, 0))
    nspec = lambda off: pl.BlockSpec((TILE, dim), lambda a, b: (b + off, 0))
    keep_rows = keep_rows or (img if img_outer else txt).shape[0]
    sspec = pl.BlockSpec(st.shape, lambda a, b: (0, 0, 0))
    in_specs = [pl.BlockSpec(memory_space=pltpu.SMEM)]
    in_specs += [ospec(i0), nspec(j0)] if img_outer else [nspec(i0), ospec(j0)]
    args = [sc, img, txt]
    alias = {}
    if stream is not None:
        alias[len(args)] = 0
        args.append(stream)
        in_specs.append(nspec(n0))
    out_off = o0 - keep_off
    if keep is not None:
        in_off = o0 if keep.shape[0] > keep_rows else out_off
        if keep.shape[0] == keep_rows:
            alias[len(args)] = 1
        args.append(keep)
        in_specs.append(ospec(in_off))
    if extra is not None:
        args.append(extra)
        in_specs.append(ospec(o0))
    alias[len(args)] = 2
    args.append(st)
    in_specs.append(sspec)
    pairs = ni * nj * TILE * TILE
    kernel = functools.partial(
        block_kernel, diag=diag, img_outer=img_outer, i0=i0, j0=j0, stream_init=stream is not None,
        keep_init=keep is not None, extra=extra is not None, fresh_from=fresh_from, spare=spare,
    )
    stream_shape = jax.ShapeDtypeStruct((txt if img_outer else img).shape, F32)
    spare_specs = [pl.BlockSpec(memory_space=pl.ANY)] if spare else []
    spare_shapes = [stream_shape] if spare else []
    return pl.pallas_call(
        kernel,
        grid=grid,
        in_specs=in_specs,
        out_specs=[nspec(n0), ospec(out_off), sspec] + spare_specs,
        out_shape=[
            stream_shape,
            jax.ShapeDtypeStruct((keep_rows, dim), F32),
            jax.ShapeDtypeStruct(st.shape, F32),
        ] + spare_shapes,
        scratch_shapes=[pltpu.VMEM((TILE, TILE), BF16)],
        input_output_aliases=alias,
        compiler_params=pltpu.CompilerParams(dimension_semantics=("arbitrary", "arbitrary"), vmem_limit_bytes=63 * 2**20),
        cost_estimate=pl.CostEstimate(flops=6 * pairs * dim, transcendentals=3 * pairs, bytes_accessed=40 * 2**20),
        name="pair_block",
    )(*args)


def solution(mesh):
    axis_name = mesh.axis_names[0]
    n_dev = mesh.shape[axis_name]

    def swap(x, bit):
        return lax.ppermute(x, axis_name, [(d, d ^ bit) for d in range(n_dev)])

    CORE, X, Y = 1, 2, 4

    def per_device(img_own, txt_own, log_temp, logit_bias):
        rows, _ = img_own.shape
        n_total = rows * n_dev
        nb = rows // TILE
        half = nb // 2
        cut = half * TILE
        scale = jnp.exp(log_temp[0])
        bias = logit_bias[0]
        over = jnp.where(scale * 1.02 + bias > CLAMP * LN2, 1.0, 0.0)
        over_own = jnp.where(scale * 1.02 - bias > CLAMP * LN2, 1.0, 0.0)
        sc = jnp.stack([scale * LOG2E, bias * LOG2E, over, over_own]).astype(F32)

        img_x = swap(img_own, X)
        txt_y = swap(txt_own, Y)
        txt_p = swap(txt_own, CORE)
        txt_yp = swap(txt_y, CORE)

        st = jnp.zeros((4, 8, 128), F32)
        back = dict(img_outer=False)

        tg_own, ig_own, st, spare = block_call(sc, img_own, txt_own, None, None, st, diag=True, irange=(0, 1), spare=True)
        ig_own, tg_p, st = block_call(sc, img_own, txt_p, ig_own, None, st, fresh_from=1, **back)
        ig_x, tg_y, st = block_call(sc, img_x, txt_y, spare, None, st, fresh_from=0, **back)
        ig_x, tg_yp, st = block_call(sc, img_x, txt_yp, ig_x, None, st, **back)
        ig_own, tg_yp, st = block_call(sc, img_own, txt_yp, ig_own, tg_yp, st, **back)
        from_yp = swap(tg_yp, CORE)
        tg_own, ig_x, st = block_call(sc, img_x, txt_own, tg_own, ig_x, st)
        tg_p, ig_x0, st = block_call(sc, img_x, txt_p, tg_p, ig_x, st, irange=(0, half), keep_rows=cut)
        from_x0 = swap(ig_x0, X)
        ig_own, tg_y0, st = block_call(sc, img_own, txt_y, ig_own, tg_y, st, jrange=(0, half), keep_rows=cut, extra=from_yp, **back)
        from_y0 = swap(tg_y0, Y)
        tg_p, ig_x1, st = block_call(sc, img_x, txt_p, tg_p, ig_x, st, irange=(half, nb), keep_rows=cut, keep_off=half)
        from_x1 = swap(ig_x1, X)
        from_p = swap(tg_p, CORE)
        last = cut - TILE
        ig_own, tg_y1, st = block_call(sc, img_own, txt_y, ig_own, tg_y, st, jrange=(half, nb - 1), keep_rows=last, keep_off=half, extra=from_yp, **back)
        from_y1 = swap(tg_y1, Y)
        ig_own, tg_y2, st = block_call(sc, img_own, txt_y, ig_own, tg_y, st, jrange=(nb - 1, nb), keep_rows=TILE, keep_off=nb - 1, extra=from_yp, **back)
        from_y2 = swap(tg_y2, Y)
        tg_own, ig_own, st = block_call(sc, img_own, txt_own, tg_own, ig_own, st, diag=True, irange=(1, nb))

        factor = scale / n_total
        img_grad = (ig_own + jnp.concatenate([from_x0, from_x1])) * factor
        txt_grad = (tg_own + from_p + jnp.concatenate([from_y0, from_y1, from_y2])) * factor
        sums = jnp.sum(st, axis=(1, 2))
        sums = lax.psum(jnp.stack([sums[0] * LN2 + sums[1], sums[2], sums[3]]), axis_name)
        return (sums[0:1] / n_total, img_grad, txt_grad, sums[2:3] * factor, sums[1:2] / n_total)

    return jax.shard_map(per_device, mesh=mesh, in_specs=(P(axis_name, None), P(axis_name, None), P(None), P(None)), out_specs=(P(None), P(axis_name, None), P(axis_name, None), P(None), P(None)), check_vma=False)
```

```python
import functools
import jax
import jax.numpy as jnp
from jax import lax
from jax.experimental import pallas as pl
from jax.experimental.pallas import tpu as pltpu
from jax.sharding import PartitionSpec as P


F32 = jnp.float32
BF16 = jnp.bfloat16
CLAMP = 31.0
LOG2E = 1.4426950408889634
LN2 = 0.6931471805599453
TILE = 1024
PIECE_M = 256
PIECE_N = 512
NN = (((1,), (0,)), ((), ()))
NT = (((1,), (1,)), ((), ()))
TN = (((0,), (0,)), ((), ()))


def dot(a, b, dims):
    return lax.dot_general(a, b, dims, preferred_element_type=F32)


def fold(x):
    m, n = x.shape
    x = jnp.sum(x.reshape(m // 8, 8, n), axis=0)
    return sum(x[:, k * 128:(k + 1) * 128] for k in range(n // 128))


def pair_terms(y, flip):
    if flip is not None:
        y = jnp.where(flip, -y, y)
    e = jnp.exp2(jnp.minimum(y, CLAMP))
    d = 1.0 + e
    c = e * (1.0 / d)
    h = e.shape[0] // 4
    e0, e1, e2, e3 = (e[k * h:(k + 1) * h] for k in range(4))
    qa = e0 * d[h:2 * h] + e1
    qb = e2 * d[3 * h:] + e3
    q = qa * (1.0 + qb) + qb
    dq = 1.0 + q
    log_part = jnp.log2(dq)
    rest_part = (q - (dq - 1.0)) * (1.0 / dq)
    if flip is not None:
        c = jnp.where(flip, -c, c)
    return c, log_part, rest_part


def block_kernel(*refs, diag, img_outer, i0, j0, stream_init, keep_init, extra, fresh_from, spare):
    it = iter(refs)
    sc_ref, img_ref, txt_ref = next(it), next(it), next(it)
    stream_in = next(it) if stream_init else None
    keep_in = next(it) if keep_init else None
    keep_extra = next(it) if extra else None
    st_in, stream_ref, keep_ref, st_ref = next(it), next(it), next(it), next(it)
    if spare:
        next(it)
    coef = next(it)
    outer, inner = pl.program_id(0), pl.program_id(1)
    i, j = (outer, inner) if img_outer else (inner, outer)
    s2 = sc_ref[0]
    b2 = sc_ref[1]

    @pl.when((outer == 0) & (inner == 0))
    def _():
        st_ref[...] = st_in[...]

    @pl.when(inner == 0)
    def _():
        base = keep_in[...] if keep_init else jnp.zeros_like(keep_ref)
        keep_ref[...] = base + keep_extra[...] if extra else base

    if fresh_from is not None:
        @pl.when((outer == 0) & (inner >= fresh_from))
        def _():
            stream_in[...] = jnp.zeros_like(stream_in)

    if img_outer:
        ig_ref, tg_ref, ig_base, tg_base = keep_ref, stream_ref, keep_ref, stream_in
    else:
        ig_ref, tg_ref, ig_base, tg_base = stream_ref, keep_ref, stream_in, keep_ref

    def flip_mask(m, n, rows, cols):
        row = lax.broadcasted_iota(jnp.int32, (rows, cols), 0) + ((i0 + i) * TILE + m)
        col = lax.broadcasted_iota(jnp.int32, (rows, cols), 1) + ((j0 + j) * TILE + n)
        return row == col

    def txt_part(n, k):
        add = dot(coef[:, n:n + PIECE_N], img_ref[:, k:k + 256], TN)
        tg_ref[n:n + PIECE_N, k:k + 256] = add if tg_base is None else tg_base[n:n + PIECE_N, k:k + 256] + add

    def tile(on_diag):
        queue = []
        for n in range(0, TILE, PIECE_N):
            for m in range(0, TILE, PIECE_M):
                dots = dot(img_ref[m:m + PIECE_M, :], txt_ref[n:n + PIECE_N, :], NT)
                flip = None
                if on_diag and m < n + PIECE_N and n < m + PIECE_M:
                    shape = (PIECE_M, PIECE_N)
                    flip = lax.broadcasted_iota(jnp.int32, shape, 0) + (m - n) == lax.broadcasted_iota(jnp.int32, shape, 1)
                c, log_part, rest_part = pair_terms(dots * s2 + b2, flip)
                coef[m:m + PIECE_M, n:n + PIECE_N] = c.astype(BF16)
                st_ref[0] += fold(log_part)
                st_ref[1] += fold(rest_part)
                st_ref[2] += fold(c)
                st_ref[3] += fold(c * dots)
                left = (TILE - m) // PIECE_M
                for _ in range((len(queue) + left - 1) // left):
                    queue.pop(0)()
            queue += [functools.partial(txt_part, n, k) for k in range(0, img_ref.shape[1], 256)]
        for task in queue:
            task()
        ig_ref[...] = ig_base[...] + dot(coef[...], txt_ref[...], NN)

    if diag:
        pl.when(i0 + i == j0 + j)(lambda: tile(True))
        pl.when(i0 + i != j0 + j)(lambda: tile(False))
    else:
        tile(False)

    @pl.when(sc_ref[2] > 0.0)
    def _():
        @pl.loop(0, TILE // 256)
        def _(k):
            m = pl.multiple_of(k * 256, 256)
            y = dot(img_ref[pl.ds(m, 256), :], txt_ref[...], NT) * s2 + b2
            if diag:
                y = jnp.where(flip_mask(m, 0, 256, TILE), 0.0, y)
            st_ref[0] += fold(jnp.maximum(y - CLAMP, 0.0))

    if diag:
        @pl.when((sc_ref[3] > 0.0) & (i0 + i == j0 + j))
        def _():
            own = jnp.sum(img_ref[...].astype(F32) * txt_ref[...].astype(F32), axis=1, keepdims=True)
            excess = jnp.maximum(-(own * s2 + b2) - CLAMP, 0.0)
            st_ref[0] += fold(jnp.broadcast_to(excess, (TILE, 128))) * (1.0 / 128.0)


def block_call(sc, img, txt, stream, keep, st, *, diag=False, img_outer=True, irange=None, jrange=None, keep_off=0, keep_rows=None, extra=None, fresh_from=None, spare=False):
    dim = img.shape[1]
    i0, i1 = irange or (0, img.shape[0] // TILE)
    j0, j1 = jrange or (0, txt.shape[0] // TILE)
    ni, nj = i1 - i0, j1 - j0
    if img_outer:
        grid, o0, n0 = (ni, nj), i0, j0
    else:
        grid, o0, n0 = (nj, ni), j0, i0
    ospec = lambda off: pl.BlockSpec((TILE, dim), lambda a, b: (a + off, 0))
    nspec = lambda off: pl.BlockSpec((TILE, dim), lambda a, b: (b + off, 0))
    keep_rows = keep_rows or (img if img_outer else txt).shape[0]
    sspec = pl.BlockSpec(st.shape, lambda a, b: (0, 0, 0))
    in_specs = [pl.BlockSpec(memory_space=pltpu.SMEM)]
    in_specs += [ospec(i0), nspec(j0)] if img_outer else [nspec(i0), ospec(j0)]
    args = [sc, img, txt]
    alias = {}
    if stream is not None:
        alias[len(args)] = 0
        args.append(stream)
        in_specs.append(nspec(n0))
    out_off = o0 - keep_off
    if keep is not None:
        in_off = o0 if keep.shape[0] > keep_rows else out_off
        if keep.shape[0] == keep_rows:
            alias[len(args)] = 1
        args.append(keep)
        in_specs.append(ospec(in_off))
    if extra is not None:
        args.append(extra)
        in_specs.append(ospec(o0))
    alias[len(args)] = 2
    args.append(st)
    in_specs.append(sspec)
    pairs = ni * nj * TILE * TILE
    kernel = functools.partial(
        block_kernel, diag=diag, img_outer=img_outer, i0=i0, j0=j0, stream_init=stream is not None,
        keep_init=keep is not None, extra=extra is not None, fresh_from=fresh_from, spare=spare,
    )
    stream_shape = jax.ShapeDtypeStruct((txt if img_outer else img).shape, F32)
    spare_specs = [pl.BlockSpec(memory_space=pl.ANY)] if spare else []
    spare_shapes = [stream_shape] if spare else []
    return pl.pallas_call(
        kernel,
        grid=grid,
        in_specs=in_specs,
        out_specs=[nspec(n0), ospec(out_off), sspec] + spare_specs,
        out_shape=[
            stream_shape,
            jax.ShapeDtypeStruct((keep_rows, dim), F32),
            jax.ShapeDtypeStruct(st.shape, F32),
        ] + spare_shapes,
        scratch_shapes=[pltpu.VMEM((TILE, TILE), BF16)],
        input_output_aliases=alias,
        compiler_params=pltpu.CompilerParams(dimension_semantics=("arbitrary", "arbitrary"), vmem_limit_bytes=63 * 2**20),
        cost_estimate=pl.CostEstimate(flops=6 * pairs * dim, transcendentals=3 * pairs, bytes_accessed=40 * 2**20),
        name="pair_block",
    )(*args)


def solution(mesh):
    axis_name = mesh.axis_names[0]
    n_dev = mesh.shape[axis_name]

    def swap(x, bit):
        return lax.ppermute(x, axis_name, [(d, d ^ bit) for d in range(n_dev)])

    CORE, X, Y = 1, 2, 4

    def per_device(img_own, txt_own, log_temp, logit_bias):
        rows, _ = img_own.shape
        n_total = rows * n_dev
        nb = rows // TILE
        half = nb // 2
        cut = half * TILE
        scale = jnp.exp(log_temp[0])
        bias = logit_bias[0]
        over = jnp.where(scale * 1.02 + bias > CLAMP * LN2, 1.0, 0.0)
        over_own = jnp.where(scale * 1.02 - bias > CLAMP * LN2, 1.0, 0.0)
        sc = jnp.stack([scale * LOG2E, bias * LOG2E, over, over_own]).astype(F32)

        img_x = swap(img_own, X)
        txt_y = swap(txt_own, Y)
        txt_p = swap(txt_own, CORE)
        txt_yp = swap(txt_y, CORE)

        st = jnp.zeros((4, 8, 128), F32)
        back = dict(img_outer=False)

        tg_own, ig_own, st, spare = block_call(sc, img_own, txt_own, None, None, st, diag=True, irange=(0, 1), spare=True)
        ig_own, tg_p, st = block_call(sc, img_own, txt_p, ig_own, None, st, fresh_from=1, **back)
        ig_x, tg_y, st = block_call(sc, img_x, txt_y, spare, None, st, fresh_from=0, **back)
        ig_x, tg_yp, st = block_call(sc, img_x, txt_yp, ig_x, None, st, **back)
        ig_own, tg_yp, st = block_call(sc, img_own, txt_yp, ig_own, tg_yp, st, **back)
        from_yp = swap(tg_yp, CORE)
        tg_own, ig_x0, st = block_call(sc, img_x, txt_own, tg_own, ig_x, st, irange=(0, half), keep_rows=cut)
        tg_p, ig_x0, st = block_call(sc, img_x, txt_p, tg_p, ig_x0, st, irange=(0, half), keep_rows=cut)
        from_x0 = swap(ig_x0, X)
        ig_own, tg_y0, st = block_call(sc, img_own, txt_y, ig_own, tg_y, st, jrange=(0, half), keep_rows=cut, extra=from_yp, **back)
        from_y0 = swap(tg_y0, Y)
        tg_own, ig_x1, st = block_call(sc, img_x, txt_own, tg_own, ig_x, st, irange=(half, nb), keep_rows=cut, keep_off=half)
        tg_p, ig_x1, st = block_call(sc, img_x, txt_p, tg_p, ig_x1, st, irange=(half, nb), keep_rows=cut, keep_off=half)
        from_x1 = swap(ig_x1, X)
        from_p = swap(tg_p, CORE)
        last = cut - TILE
        ig_own, tg_y1, st = block_call(sc, img_own, txt_y, ig_own, tg_y, st, jrange=(half, nb - 1), keep_rows=last, keep_off=half, extra=from_yp, **back)
        from_y1 = swap(tg_y1, Y)
        ig_own, tg_y2, st = block_call(sc, img_own, txt_y, ig_own, tg_y, st, jrange=(nb - 1, nb), keep_rows=TILE, keep_off=nb - 1, extra=from_yp, **back)
        from_y2 = swap(tg_y2, Y)
        tg_own, ig_own, st = block_call(sc, img_own, txt_own, tg_own, ig_own, st, diag=True, irange=(1, nb))

        factor = scale / n_total
        img_grad = (ig_own + jnp.concatenate([from_x0, from_x1])) * factor
        txt_grad = (tg_own + from_p + jnp.concatenate([from_y0, from_y1, from_y2])) * factor
        sums = jnp.sum(st, axis=(1, 2))
        sums = jnp.stack([sums[0] * LN2 + sums[1], sums[2], sums[3]])
        sums = sums + swap(sums, CORE)
        sums = sums + swap(sums, X)
        sums = sums + swap(sums, Y)
        return (sums[0:1] / n_total, img_grad, txt_grad, sums[2:3] * factor, sums[1:2] / n_total)

    return jax.shard_map(per_device, mesh=mesh, in_specs=(P(axis_name, None), P(axis_name, None), P(None), P(None)), out_specs=(P(None), P(axis_name, None), P(axis_name, None), P(None), P(None)), check_vma=False)
```
